256 devices in a mesh: row: 16 (over z_hi, y, core), col: 16 (over x, z_lo).
Axes of the slice: x: 4, y: 4, z: 8 (z_hi: 2, z_lo: 4; z = z_hi * 4 + z_lo), core: 2. Of those that a mesh axis runs over, the one named last changes fastest.
Arguments:
- series: float32 [16384, 2048], P(('row', 'col'))
- lengths: int32 [16384], P(('row', 'col')), may hold values from 512 to 2048
- starts: int32 [16384], P(('row', 'col')), may hold values from 0 to 1536, as said below
Outputs:
- correlation: float32 [16384, 16384], P('row', 'col')
The draws below stay inside these ranges and needn't reach their ends.
Inputs may be any that keep to these rules, and one draw needn't show every extreme that they name: starts[s] + lengths[s] <= 2048 for every series.
All inputs are finite; a program needn't handle non-finite values.
Results may differ from the reference program's by a relative error of at most 0.0012.
Values may be sent and summed in bfloat16 or wider, within the bound.
No kernel may reach another device: no remote copies, remote signals or barrier semaphores. Data moves between devices by JAX's collectives and lax.ppermute only.
A program may use at most 64 MiB of HBM per device.

```python
import math
import jax
import jax.numpy as jnp
from jax import lax

STEPS = 2048
SERIES = 16384
N_ROW = 16


factor_total = 24


def draw_series(key, part):
    subkeys = jax.random.split(jax.random.fold_in(key, 11), 6)
    factors = jax.random.normal(subkeys[0], (factor_total, STEPS), jnp.float32)
    loadings = jax.random.normal(subkeys[1], (SERIES, factor_total), jnp.float32)
    common = jnp.dot(loadings, factors) / math.sqrt(factor_total)
    column_scale = jnp.exp(jax.random.uniform(subkeys[2], (1, STEPS), jnp.float32, 0.0, math.log(3.0)))
    noise = jax.random.normal(subkeys[3], (SERIES, STEPS), jnp.float32)
    level = jax.random.uniform(subkeys[4], (SERIES, 1), jnp.float32, -3.0, 3.0)
    row_scale = jnp.exp(jax.random.uniform(subkeys[5], (SERIES, 1), jnp.float32, 0.0, math.log(10.0)))
    values = level + row_scale * column_scale * (common + 0.7 * noise)
    return values.astype(jnp.float32)


def windows(key):
    subkeys = jax.random.split(jax.random.fold_in(key, 7), 4)
    lengths = jax.random.randint(subkeys[0], (SERIES,), STEPS // 4, STEPS + 1, jnp.int32)
    longest = jax.random.randint(subkeys[1], (), 0, SERIES // 2, jnp.int32)
    shortest = SERIES // 2 + jax.random.randint(subkeys[2], (), 0, SERIES // 2, jnp.int32)
    lengths = lengths.at[longest].set(STEPS).at[shortest].set(STEPS // 4)
    raw_bits = jax.random.randint(subkeys[3], (SERIES,), 0, 1 << 30, jnp.int32)
    starts = raw_bits % (STEPS - lengths + 1)
    starts = starts.at[shortest].set(STEPS - STEPS // 4)
    return (lengths, starts)


def draw_lengths(key, part):
    return windows(key)[0]


def draw_starts(key, part):
    return windows(key)[1]


def setup_inputs(seed: int = 0) -> dict:
    key_of = jax.random.split(jax.random.key(seed), 4)
    return {
        "series": draw_series(jax.random.fold_in(key_of[3], 71), 0),
        "lengths": draw_lengths(jax.random.fold_in(key_of[3], 71), 0),
        "starts": draw_starts(jax.random.fold_in(key_of[3], 71), 0),
    }


def normalize(series, lengths, starts):
    positions = jnp.arange(series.shape[1], dtype=jnp.int32)[None, :]
    inside = ((positions >= starts[:, None]) & (positions < (starts + lengths)[:, None])).astype(jnp.float32)
    valid_count = lengths.astype(jnp.float32)[:, None]
    average = lax.optimization_barrier(jnp.sum(inside * series, axis=1, keepdims=True)) / valid_count
    centered = inside * (series - average)
    variance = lax.optimization_barrier(jnp.sum(centered * centered, axis=1, keepdims=True)) / valid_count
    return (centered / jnp.sqrt(valid_count * (variance + 1e-06))).astype(jnp.bfloat16)

def reference(series, lengths, starts):
    normed = normalize(series, lengths, starts)
    block_rows = SERIES // N_ROW
    blocks = normed.reshape(N_ROW, block_rows, STEPS)

    def one_block(rows_block):
        return lax.dot_general(rows_block, normed, (((1,), (1,)), ((), ())), preferred_element_type=jnp.float32)
    return lax.map(one_block, blocks).reshape(SERIES, SERIES)
```

```python
from itertools import product

import jax
import jax.numpy as jnp
from jax import lax
from jax.experimental import pallas as pl
from jax.experimental.pallas import tpu as pltpu
from jax.sharding import Mesh
from jax.sharding import PartitionSpec as P

AXES = ("zh", "y", "k", "x", "zl")
SIZES = (2, 4, 2, 4, 4)


def linear(zh, y, k, x, zl):
    return (((zh * 4 + y) * 2 + k) * 4 + x) * 4 + zl


def moved(value, target):
    places = product(*(range(n) for n in SIZES))
    pairs = [(linear(*p), linear(*target(*p))) for p in places]
    return lax.ppermute(value, AXES, pairs)


def along_x(step):
    return lambda zh, y, k, x, zl: (zh, y, k, (x + step) % 4, zl)


def along_y(step):
    return lambda zh, y, k, x, zl: (zh, (y + step) % 4, k, x, zl)


def along_z(flip):
    return lambda zh, y, k, x, zl: (zh, y, k, x, zl ^ flip)


def other_core(zh, y, k, x, zl):
    return (zh, y, 1 - k, x, zl)


def to_column(turn):
    def target(zh, y, k, x, zl):
        half = zh if (zl & 1) == turn else 1 - zh
        return (half, x, zl >> 1, 2 * zh + (y >> 1), 2 * (y & 1) + k)

    return target


def normalize_kernel(series_ref, window_ref, out_ref):
    series = series_ref[...]
    starts, lengths = window_ref[:, 0:1], window_ref[:, 1:2]
    positions = lax.broadcasted_iota(jnp.int32, series.shape, 1)
    inside = (positions >= starts) & (positions < starts + lengths)
    valid_count = lengths.astype(jnp.float32)
    average = jnp.sum(jnp.where(inside, series, 0.0), axis=1, keepdims=True) / valid_count
    centered = jnp.where(inside, series - average, 0.0)
    variance = jnp.sum(centered * centered, axis=1, keepdims=True) / valid_count
    normed = centered / jnp.sqrt(valid_count * (variance + 1e-06))
    out_ref[...] = normed.astype(out_ref.dtype)


def normalize(series, lengths, starts):
    rows, steps = series.shape
    block = 16
    return pl.pallas_call(
        normalize_kernel,
        grid=(rows // block,),
        in_specs=[
            pl.BlockSpec((block, steps), lambda i: (i, 0)),
            pl.BlockSpec((block, 2), lambda i: (i, 0)),
        ],
        out_specs=pl.BlockSpec((block, steps), lambda i: (i, 0)),
        out_shape=jax.ShapeDtypeStruct((rows, steps), jnp.bfloat16),
        cost_estimate=pl.CostEstimate(
            flops=12 * rows * steps, bytes_accessed=6 * rows * steps, transcendentals=0
        ),
        name="normalize",
    )(series, jnp.stack([starts, lengths], axis=1))


def place_of(device):
    zl, x, k, y, zh = device & 3, (device >> 2) & 3, (device >> 4) & 1, (device >> 5) & 3, device >> 7
    return zh, y, k, x, zl


def row_group(device, shift):
    return (place_of(device)[3] - shift) & 3


def row_slot(device, flip):
    return place_of(device)[4] ^ flip


def col_slot(device, swapped, turn, shift):
    zh, y, k, x, _ = place_of(device)
    return 4 * ((y - shift) & 3) + 2 * (k ^ swapped) + (turn ^ zh ^ (x >> 1))


def correlate_kernel(device_ref, *refs):
    pieces, out_ref = refs[:32], refs[32]
    left, right, left_sem, right_sem = refs[33:]
    group = pl.program_id(0)
    size = pieces[0].shape[0]
    device = device_ref[0]

    def left_copy(i):
        slot = pl.ds(pl.multiple_of(row_slot(device, i % 4) * size, size), size)
        return pltpu.make_async_copy(pieces[i], left.at[i // 4, slot], left_sem.at[i])

    def right_copy(i):
        place = col_slot(device, i // 8, (i // 4) % 2, i % 4)
        slot = pl.ds(pl.multiple_of(place * size, size), size)
        return pltpu.make_async_copy(pieces[16 + i], right.at[slot], right_sem.at[i])

    @pl.when(group == 0)
    def _():
        for i in range(4):
            left_copy(i).start()
        for i in range(16):
            right_copy(i).start()
        for i in range(4, 16):
            left_copy(i).start()
        for i in range(16):
            right_copy(i).wait()

    for g in range(4):

        @pl.when(group == g)
        def _():
            for i in range(4 * g, 4 * g + 4):
                left_copy(i).wait()

    out_ref[...] = lax.dot_general(
        left[group], right[...], (((1,), (1,)), ((), ())), preferred_element_type=jnp.float32
    )


def correlate(rows, cols):
    size, steps = rows[0].shape
    device = lax.axis_index(AXES).reshape(1)
    flops = 2 * (16 * size) ** 2 * steps
    return pl.pallas_call(
        correlate_kernel,
        grid_spec=pltpu.PrefetchScalarGridSpec(
            num_scalar_prefetch=1,
            grid=(4,),
            in_specs=[pl.BlockSpec(memory_space=pl.ANY)] * 32,
            out_specs=pl.BlockSpec(
                (4 * size, 16 * size), lambda g, device: (row_group(device[0], g), 0)
            ),
            scratch_shapes=[
                pltpu.VMEM((4, 4 * size, steps), jnp.bfloat16),
                pltpu.VMEM((16 * size, steps), jnp.bfloat16),
                pltpu.SemaphoreType.DMA((16,)),
                pltpu.SemaphoreType.DMA((16,)),
            ],
        ),
        out_shape=jax.ShapeDtypeStruct((16 * size, 16 * size), jnp.float32),
        cost_estimate=pl.CostEstimate(
            flops=flops, bytes_accessed=12 * 2**20, transcendentals=0
        ),
        compiler_params=pltpu.CompilerParams(vmem_limit_bytes=24 * 2**20),
        name="correlate",
    )(device, *rows, *cols)


def ring_gather(first, second, along):
    first_low, first_high = moved(first, along(1)), moved(first, along(-1))
    second_low, second_high = moved(second, along(1)), moved(second, along(-1))
    first_far = moved(first_low, along(1))
    second_far = moved(second_high, along(-1))
    return [first, first_low, first_far, first_high], [second, second_low, second_far, second_high]


def on_device(series, lengths, starts):
    normed = normalize(series, lengths, starts)

    arrived = [moved(normed, to_column(turn)) for turn in range(2)]
    near = [normed] + [moved(normed, along_z(m)) for m in (1, 2, 3)]

    cols = ring_gather(arrived[0], arrived[1], along_y)
    cols = cols[0] + cols[1]
    cols = cols + [moved(p, other_core) for p in cols]

    by_near = []
    for a, b in ((0, 1), (2, 3)):
        by_near += ring_gather(near[a], near[b], along_x)
    rows = [by_near[m][s] for s in range(4) for m in range(4)]

    return correlate(rows, cols)


def solution(mesh):
    split = Mesh(mesh.devices.reshape(SIZES), AXES)
    placed = (P(AXES, None), P(AXES), P(AXES))
    return jax.shard_map(
        on_device,
        mesh=split,
        in_specs=placed,
        out_specs=P(("zh", "y", "k"), ("x", "zl")),
        check_vma=False,
    )
```
